32 devices in a mesh: dp: 4 (over y, x), expert: 8 (over z, core).
Axes of the slice: x: 2, y: 2, z: 4, core: 2. Of those that a mesh axis runs over, the one named last changes fastest.
Arguments:
- tokens: bfloat16 [4096, 4096], P(('dp', 'expert')), may hold values from -6 to 6
- routes: int32 [4096, 2], P(('dp', 'expert')), may hold values from 0 to 7, all different within a row; in each aligned block of 128 rows (0 to 127, 128 to 255, ...) at most 48 rows name the same one
- router_weight: bfloat16 [4096, 8], replicated, may hold values from -0.09375 to 0.09375
- shift: float32 [1, 4096], replicated, may hold values from -3 to 3
- scale: float32 [1, 4096], replicated, may hold values from -3 to 3
- gate_mod: float32 [1, 4096], replicated, may hold values from -4 to 4
- gate_weight: bfloat16 [8, 4096, 1024], P(None, ('dp', 'expert')), may hold values from -0.09375 to 0.09375
- up_weight: bfloat16 [8, 4096, 1024], P(None, ('dp', 'expert')), may hold values from -0.09375 to 0.09375
- down_weight: bfloat16 [8, 4096, 1024], P(None, ('dp', 'expert')), may hold values from -0.1875 to 0.1875
Outputs:
- update: bfloat16 [4096, 4096], P(('dp', 'expert'))
The draws below stay inside these ranges and needn't reach their ends.
Inputs may be any that keep to these rules, and one draw needn't show every extreme that they name: `routes`: each row names two different experts; among the rows of one device no expert is named more than 48 times, a bound that some block reaches.
All inputs are finite; a program needn't handle non-finite values.
Results may differ from the reference program's by a relative error of at most 0.0072.
Values may be sent and summed in bfloat16 or wider, within the bound.
A program may use at most 128 MiB of HBM per device.

```python
import math
import jax
import jax.numpy as jnp
import numpy as np
from jax import lax

D = 4096
FE = 1024
E = 8
TOK_DEV = 128
CAP = 48
PIX = 4096
TOKENS = 4096
IMAGES = 1


def steps_of(key, extent, cuts, least, high):
    level, own = 1.0, jax.random.fold_in(key, 6)
    for dim, blocks in cuts:
        steps = jnp.exp(jax.random.uniform(jax.random.fold_in(own, dim), (blocks,), jnp.float32, least / len(cuts), high / len(cuts)))
        level = level * jnp.repeat(steps, extent[dim] // blocks).reshape([-1 if axis == dim else 1 for axis in range(len(extent))])
    return level


def routed_block(rng, own, number, rows, count, top, limit, skew):
    order = jax.random.permutation(rng, count)
    crowded, usual = shares(count, rows * top, limit, skew, True), shares(count, rows * top, limit, skew, False)
    places = jnp.arange(count)

    def named(tallies, turn):
        used = int((tallies > 0).sum())
        fixed = max(1, used // 4)
        moved = fixed + (places - fixed + turn * (used - fixed)) % max(1, count - fixed)
        return jnp.zeros((count,), jnp.int32).at[order[jnp.where(places < fixed, places, moved)]].set(jnp.asarray(tallies, jnp.int32))

    tallies = jnp.where(number % 4 == 0, named(crowded, number // 4), named(usual, number - number // 4 - 1))
    mixed = jax.random.permutation(jax.random.fold_in(own, 3), count)
    donor, receiver = mixed[0:count // 2 * 2:2], mixed[1:count // 2 * 2:2]
    margin = jnp.minimum(tallies[donor] - 1, limit - tallies[receiver]) // 2
    margin = jnp.where((donor == order[0]) | (receiver == order[0]) | (tallies[receiver] == 0), 0, jnp.maximum(margin, 0))
    moved = jax.random.randint(jax.random.fold_in(own, 4), (count // 2,), 0, 1 << 20) % (margin + 1)
    tallies = tallies.at[donor].add(-moved).at[receiver].add(moved)
    labels = jnp.searchsorted(jnp.cumsum(tallies), jnp.arange(rows * top), side="right").astype(jnp.int32)
    listing = labels.reshape(top, rows).T
    listing = listing[jax.random.permutation(jax.random.fold_in(own, 1), rows)]
    turn = jax.random.randint(jax.random.fold_in(own, 2), (rows, 1), 0, top)
    return jnp.take_along_axis(listing, (jnp.arange(top)[None, :] + turn) % top, axis=1)


def shares(number_of, total, reach, lean, full):
    loads = [(1 << 20) // math.isqrt(rank ** lean) + 1 for rank in range(1, number_of + 1)]
    largest = reach if full else min(reach, max(-(-total // number_of), total * loads[0] // sum(loads)))
    least = 1 if total - largest >= number_of - 1 else 0
    given, rest = [largest] + [least] * (number_of - 1), total - largest - least * (number_of - 1)
    while rest > 0:
        candidates = [i for i in range(1, number_of) if given[i] < largest] or [i for i in range(1, number_of) if given[i] < reach]
        mass, budget = sum([loads[i] for i in candidates]), rest
        for i in candidates:
            addition = min(reach - given[i], max(1, budget * loads[i] // mass), rest)
            given[i] = given[i] + addition
            rest = rest - addition
    return np.array(given)


def gaussian(rng, shape, scale, bound, pieces=(), kind=jnp.bfloat16):
    factor_of = steps_of(rng, shape, pieces, -0.22, 0.18) if pieces else 1.0
    result = jax.random.normal(rng, shape, jnp.float32) * scale * factor_of
    return jnp.minimum(jnp.maximum(result, -bound), bound).astype(kind)


def setup_inputs(seed: int = 0) -> dict:
    arg_keys = jax.random.split(jax.random.key(seed), 10)
    tokens = gaussian(arg_keys[0], (TOKENS, D), 1.0, 6.0, ((0, 32),))
    routes_keys = jax.random.split(jax.random.fold_in(arg_keys[1], 1), TOKENS // TOK_DEV)
    routes_turns = jax.random.permutation(jax.random.fold_in(arg_keys[1], 3), TOKENS // TOK_DEV)
    routes = jax.vmap(lambda own, number: routed_block(jax.random.fold_in(arg_keys[1], 2), own, number, TOK_DEV, E, 2, CAP, 2))(routes_keys, routes_turns).reshape((TOKENS, 2))
    router_weight = gaussian(arg_keys[2], (D, E), D ** -0.5, 0.09375)
    shift = gaussian(arg_keys[3], (IMAGES, D), 0.5, 3.0, (), jnp.float32)
    scale = gaussian(arg_keys[4], (IMAGES, D), 0.5, 3.0, (), jnp.float32)
    gate_mod = gaussian(arg_keys[5], (IMAGES, D), 1.0, 4.0, (), jnp.float32)
    gate_weight = gaussian(arg_keys[6], (E, D, FE), D ** -0.5, 0.09375, ((1, 32),))
    up_weight = gaussian(arg_keys[7], (E, D, FE), D ** -0.5, 0.09375, ((1, 32),))
    down_weight = gaussian(arg_keys[8], (E, D, FE), FE ** -0.5, 0.1875, ((1, 32),))
    return dict(tokens=tokens, routes=routes, router_weight=router_weight, shift=shift, scale=scale, gate_mod=gate_mod, gate_weight=gate_weight, up_weight=up_weight, down_weight=down_weight)


EPS = 1e-06

def reference(tokens, routes, router_weight, shift, scale, gate_mod, gate_weight, up_weight, down_weight):
    blocks = TOKENS // TOK_DEV

    def norm_image(items):
        rows, image_shift, image_scale = items
        values = rows.astype(jnp.float32)
        meansq = lax.optimization_barrier(jnp.mean(values * values, axis=-1, keepdims=True))
        normed_rows = values * lax.rsqrt(meansq + EPS) * (1.0 + image_scale[None, :]) + image_shift[None, :]
        normed_rows = normed_rows.astype(jnp.bfloat16)
        logit_rows = jnp.dot(normed_rows, router_weight, preferred_element_type=jnp.float32)
        return (normed_rows, logit_rows)
    normed, logits = lax.map(norm_image, (tokens.reshape(IMAGES, PIX, D), shift, scale))
    normed = normed.reshape(TOKENS, D)
    logits = logits.reshape(TOKENS, E)
    chosen = jnp.take_along_axis(logits, routes, axis=1)
    score_flat = jax.nn.sigmoid(chosen).reshape(-1)
    flat = routes.reshape(blocks, 2 * TOK_DEV)
    hot = (flat[:, :, None] == jnp.arange(E, dtype=jnp.int32)[None, None, :]).astype(jnp.int32)
    rank = (jnp.cumsum(hot, axis=1) - hot).astype(jnp.int32)
    slot = lax.optimization_barrier(jnp.sum(rank * hot, axis=-1)).astype(jnp.int32)
    position = (flat * CAP + slot).astype(jnp.int32)
    global_ids = (jnp.arange(blocks, dtype=jnp.int32)[:, None] * (2 * TOK_DEV) + jnp.arange(2 * TOK_DEV, dtype=jnp.int32)[None, :]).astype(jnp.int32)

    def fill_table(where_to, ids):
        return jnp.full((E * CAP,), -1, jnp.int32).at[where_to].set(ids)
    table = jax.vmap(fill_table)(position, global_ids)
    table = table.reshape(blocks, E, CAP).transpose(1, 0, 2).reshape(E, blocks * CAP)

    def expert_step(total, items):
        ids, w_gate, w_up, w_down = items
        filled = ids >= 0
        safe = jnp.where(filled, ids, 0).astype(jnp.int32)
        token_ids = (safe // 2).astype(jnp.int32)
        rows = jnp.where(filled[:, None], normed[token_ids], jnp.zeros((), jnp.bfloat16))
        gate = jnp.dot(rows, w_gate, preferred_element_type=jnp.float32)
        upper = jnp.dot(rows, w_up, preferred_element_type=jnp.float32)
        hidden = (jax.nn.silu(gate) * upper).astype(jnp.bfloat16)
        output = jnp.dot(hidden, w_down.T, preferred_element_type=jnp.float32).astype(jnp.bfloat16)
        weight = jnp.where(filled, score_flat[safe], jnp.zeros((), jnp.float32))
        total = total.at[token_ids].add(weight[:, None] * output.astype(jnp.float32))
        return (total, None)
    total, unused = lax.scan(expert_step, jnp.zeros((TOKENS, D), jnp.float32), (table, gate_weight, up_weight, down_weight))
    update = total.reshape(IMAGES, PIX, D) * gate_mod[:, None, :]
    return update.reshape(TOKENS, D).astype(jnp.bfloat16)
```

```python
import functools

import jax
import jax.numpy as jnp
from jax import lax
from jax.experimental import pallas as pl
from jax.experimental.pallas import tpu as pltpu
from jax.sharding import PartitionSpec as P

PIX = 4096


EPS = 1e-06

ROWS = 32
LAG_B, LAG_C, LAG_G = 3, 4, 5
LAG_R1, LAG_R2, LAG_R3 = 6, 7, 8
LAG_M, LAG_O1, LAG_O2, LAG_O3 = 11, 12, 13, 14
DOWN_AT = 2


def send_back(output):
    return lax.all_to_all(output, "expert", split_axis=0, concat_axis=0, tiled=True)


def shards_plain(
    tokens, routes, router_weight, shift, scale, gate_mod, gate_weight, up_weight, down_weight
):
    tok_dev = tokens.shape[0]
    width = tokens.shape[1]
    experts = router_weight.shape[1]
    n_owner = lax.axis_size("expert")
    local_count = experts // n_owner
    capacity = max(2, 3 * tok_dev // experts)
    first_row = (lax.axis_index("dp") * n_owner + lax.axis_index("expert")) * tok_dev
    image = first_row // PIX
    shift_row = lax.dynamic_slice_in_dim(shift, image, 1, 0)
    scale_row = lax.dynamic_slice_in_dim(scale, image, 1, 0)
    gate_row = lax.dynamic_slice_in_dim(gate_mod, image, 1, 0)
    values = tokens.astype(jnp.float32)
    meansq = jnp.mean(values * values, axis=-1, keepdims=True)
    normed = (values * lax.rsqrt(meansq + EPS) * (1.0 + scale_row) + shift_row).astype(jnp.bfloat16)
    logits = jnp.dot(normed, router_weight, preferred_element_type=jnp.float32)
    onehot = routes[:, :, None] == jnp.arange(experts, dtype=jnp.int32)[None, None, :]
    chosen = jnp.sum(jnp.where(onehot, logits[:, None, :], 0.0), axis=-1)
    score = jax.nn.sigmoid(chosen)
    flat = routes.reshape(-1)
    hot = (flat[:, None] == jnp.arange(experts, dtype=jnp.int32)[None, :]).astype(jnp.int32)
    rank = jnp.cumsum(hot, axis=0) - hot
    slot = jnp.sum(rank * hot, axis=-1)
    position = flat * capacity + slot
    source = (
        jnp.zeros((experts * capacity,), jnp.int32)
        .at[position]
        .set(jnp.arange(2 * tok_dev, dtype=jnp.int32) // 2)
    )
    filled = jnp.zeros((experts * capacity,), jnp.bool_).at[position].set(True)
    outgoing = jnp.where(filled[:, None], normed[source], jnp.zeros((), jnp.bfloat16)).reshape(
        experts, capacity, width
    )
    quarter_gate, quarter_up, quarter_down = (
        lax.all_to_all(gate_weight, "expert", split_axis=0, concat_axis=1, tiled=True),
        lax.all_to_all(up_weight, "expert", split_axis=0, concat_axis=1, tiled=True),
        lax.all_to_all(down_weight, "expert", split_axis=0, concat_axis=1, tiled=True),
    )
    w_gate, w_up, w_down = (
        lax.all_gather(quarter_gate, "dp", axis=1, tiled=True),
        lax.all_gather(quarter_up, "dp", axis=1, tiled=True),
        lax.all_gather(quarter_down, "dp", axis=1, tiled=True),
    )
    received = lax.all_to_all(outgoing, "expert", split_axis=0, concat_axis=0, tiled=True)
    slots = received.shape[1]
    grid = received.reshape(n_owner, local_count, slots, width)
    gate = jnp.einsum("nxcd,xdf->nxcf", grid, w_gate, preferred_element_type=jnp.float32)
    upper = jnp.einsum("nxcd,xdf->nxcf", grid, w_up, preferred_element_type=jnp.float32)
    hidden = (jax.nn.silu(gate) * upper).astype(jnp.bfloat16)
    output = jnp.einsum(
        "nxcf,xdf->nxcd", hidden, w_down, preferred_element_type=jnp.float32
    ).astype(jnp.bfloat16)
    output = output.reshape(n_owner * local_count, slots, width)
    incoming = send_back(output)
    picked = (
        incoming.reshape(experts * capacity, width)[position]
        .astype(jnp.float32)
        .reshape(tok_dev, 2, width)
    )
    branch = jnp.sum(score[:, :, None] * picked, axis=1)
    return (gate_row * branch).astype(jnp.bfloat16)


MESH = pl.DeviceIdType.MESH
F32, BF16 = jnp.float32, jnp.bfloat16


def wait_bytes(ref, sem):
    pltpu.make_async_copy(ref, ref, sem).wait()


def kernel(
    tok_ref, router_ref, routes_ref, shift_ref, scale_ref, gmod_ref, gate_ref, up_ref, down_ref, out_ref,
    pieces, grid, weights, downs, meta, facts_col, part, from_outer, summed, from_mid, hidden, masked,
    sums, from_core, added, from_first, paired, from_second, final, land, gmod_z,
    sent, w_recv, m_recv, z_recv, x_recv, y_recv, d_recv, c_recv, o_recv, mid_recv, h_recv,
    core_recv, first_recv, second_recv, out_recv,
):
    dp, me = lax.axis_index("dp"), lax.axis_index("expert")
    n_z = pieces.shape[0]
    z, c = me // 2, me % 2
    x, y = dp % 2, dp // 2
    x_dp, y_dp, d_dp = dp + 1 - 2 * x, dp + 2 - 4 * y, 3 - dp
    mate = me + 1 - 2 * c
    spot, x_spot, y_spot, d_spot = dp * 2 + c, x_dp * 2 + c, y_dp * 2 + c, d_dp * 2 + c
    tok_dev, width = tok_ref.shape
    experts, depth, units = gate_ref.shape
    chunks, n_spot, rows, dset = grid.shape
    n_j = tok_dev // rows
    block = depth
    unit = units // n_spot
    n_dp = n_spot // 2

    def remote(src, dst, send_sem, recv_sem, to):
        return pltpu.make_async_remote_copy(
            src_ref=src, dst_ref=dst, send_sem=send_sem, recv_sem=recv_sem, device_id=to, device_id_type=MESH
        )

    barrier = pltpu.get_barrier_semaphore()
    for t in range(1, n_spot):
        to = (spot + t) % n_spot
        pl.semaphore_signal(barrier, inc=1, device_id=(to // 2, z * 2 + to % 2), device_id_type=MESH)
    for t in range(1, n_z):
        for k in range(2):
            pl.semaphore_signal(barrier, inc=1, device_id=(dp, ((z + t) % n_z) * 2 + k), device_id_type=MESH)
    pl.semaphore_wait(barrier, n_spot - 1 + 2 * (n_z - 1))

    def own_rows(ref, w):
        return ref.at[:, pl.ds(pl.multiple_of(w * block, block), block), :]

    def send_weight(a):
        ref = (gate_ref, up_ref)[a]
        mine = weights.at[:, pl.ds(pl.multiple_of(spot * block, block), block), a * unit : (a + 1) * unit]

        def source(s):
            return ref.at[:, :, pl.ds(pl.multiple_of(s * unit, unit), unit)]

        pltpu.make_async_copy(source(spot), mine, w_recv.at[a]).start()
        for s in (x_dp * 2 + c, y_dp * 2 + 1 - c, d_dp * 2 + c, y_dp * 2 + c, x_dp * 2 + 1 - c, d_dp * 2 + 1 - c, dp * 2 + 1 - c):
            remote(source(s), mine, sent.at[a], w_recv.at[a], (s // 2, z * 2 + s % 2)).start()

    def send_down(e):
        mine = downs.at[
            pl.ds(pl.multiple_of(spot * block, block), block), pl.ds(pl.multiple_of(e * unit, unit), unit)
        ]

        def source(s):
            return down_ref.at[e, :, pl.ds(pl.multiple_of(s * unit, unit), unit)]

        pltpu.make_async_copy(source(spot), mine, w_recv.at[2]).start()
        for s in (x_dp * 2 + c, y_dp * 2 + 1 - c, d_dp * 2 + c, y_dp * 2 + c, x_dp * 2 + 1 - c, d_dp * 2 + 1 - c, dp * 2 + 1 - c):
            remote(source(s), mine, sent.at[2], w_recv.at[2], (s // 2, z * 2 + s % 2)).start()

    send_weight(0)

    fine = 16
    wide = 2 * block

    def home(z_to, d):
        return (d * n_z + z_to) * wide

    @pl.loop(0, n_j)
    def _(j):
        for b in range(rows // fine):
            at = pl.ds(pl.multiple_of(j * rows + b * fine, fine), fine)
            values = tok_ref[at, :].astype(F32)
            meansq = jnp.mean(values * values, axis=-1, keepdims=True)
            fresh = (values * lax.rsqrt(meansq + EPS) * (1.0 + scale_ref[...]) + shift_ref[...]).astype(BF16)
            for t in range(n_z):
                for d in range(n_dp):
                    pieces[t, at, d * wide : (d + 1) * wide] = fresh[:, home(t, d) : home(t, d) + wide]
        span = pl.ds(pl.multiple_of(j * rows, rows), rows)
        grid[j * n_z + z, spot] = pieces[z, span, :]
        for t in range(1, n_z):
            to = (z + t) % n_z
            remote(
                pieces.at[to, span, :], grid.at[j * n_z + z, spot], sent.at[3], z_recv.at[j * n_z + z], (dp, to * 2 + c)
            ).start()

    logits = jnp.zeros((tok_dev, experts), F32)
    for t in range(n_z):
        for d in range(n_dp):
            logits += jnp.dot(
                pieces[t, :, d * wide : (d + 1) * wide], router_ref[home(t, d) : home(t, d) + wide, :],
                preferred_element_type=F32,
            )
    names = lax.broadcasted_iota(jnp.int32, logits.shape, 1)
    lanes = lax.broadcasted_iota(jnp.int32, (tok_dev, 128), 1)
    facts = jnp.zeros((tok_dev, 128), F32)
    for k in range(2):
        chosen = jnp.sum(jnp.where(routes_ref[:, k : k + 1] == names, logits, 0.0), axis=-1, keepdims=True)
        facts = jnp.where(lanes == k, routes_ref[:, k : k + 1].astype(F32), facts)
        facts = jnp.where(lanes == 2 + k, jax.nn.sigmoid(chosen), facts)
    meta[me, dp] = facts.T[0:8, :]
    for to in (x_dp, y_dp, d_dp):
        remote(meta.at[me, dp], meta.at[me, dp], sent.at[4], m_recv.at[0], (to, me)).start()
    send_weight(1)
    for d in range(n_dp):
        gmod_z[:, d * wide : (d + 1) * wide] = gmod_ref[
            :, pl.ds(pl.multiple_of((d * n_z + z) * wide, wide), wide)
        ]
    wait_bytes(meta.at[me, pl.ds(0, n_dp - 1)], m_recv.at[0])
    for t in range(1, 2 * n_z):
        remote(meta.at[me], meta.at[me], sent.at[5], m_recv.at[1], (dp, (me + t) % (2 * n_z))).start()
    wait_bytes(meta.at[pl.ds(0, 2 * n_z - 1)], m_recv.at[1])

    @pl.loop(0, 2 * n_z)
    def _(e):
        for d in range(n_dp):
            column = meta[e, d].T
            for j in range(n_j):
                at = pl.ds(pl.multiple_of((d * 2 + e % 2) * rows, rows), rows)
                facts_col[j * n_z + e // 2, at, :] = column[j * rows : (j + 1) * rows, :]

    def stage_a(i):
        held = grid.at[i, spot]

        @pl.when(i % n_z != z)
        def _():
            wait_bytes(held, z_recv.at[i])

        remote(held, held, sent.at[6], x_recv.at[i], (x_dp, me)).start()
        remote(held, held, sent.at[6], y_recv.at[i], (y_dp, me)).start()
        remote(held, held, sent.at[6], c_recv.at[i], (dp, mate)).start()

    def stage_b(i):
        par = (i // n_z + i) % 2
        wait_bytes(grid.at[i, x_spot], x_recv.at[i])
        wait_bytes(grid.at[i, y_spot], y_recv.at[i])
        relayed = grid.at[i, x_spot + par * (y_spot - x_spot)]
        remote(relayed, relayed, sent.at[7], d_recv.at[i], (y_dp + par * (x_dp - y_dp), me)).start()
        for s in (x_spot, y_spot):
            remote(grid.at[i, s], grid.at[i, s], sent.at[7], c_recv.at[i], (dp, mate)).start()

    def stage_c(i):
        held = grid.at[i, d_spot]
        wait_bytes(held, d_recv.at[i])
        remote(held, held, sent.at[8], c_recv.at[i], (dp, mate)).start()

    total = n_spot * rows
    mid_f = 2 - z
    out_f = 1 - z // 3

    def stage_g(i):
        @pl.when(i == 0)
        def _():
            for a in range(2):
                wait_bytes(weights.at[:, :, a * unit : (a + 1) * unit], w_recv.at[a])

        wait_bytes(grid.at[i, pl.ds(0, n_dp)], c_recv.at[i])
        block_in = grid[i].reshape(total, dset)
        first = facts_col[i, :, 0:1]
        second = facts_col[i, :, 1:2]
        picked = [jnp.zeros((total, 2 * unit), F32)] * 2
        for e in range(experts):
            result = jnp.dot(block_in, weights[e], preferred_element_type=F32)
            picked = [jnp.where(who == float(e), result, old) for who, old in zip((first, second), picked)]
        for k in range(2):
            part[i, k] = picked[k].astype(BF16)

        @pl.when(z % 3 == 0)
        def _():
            to = (dp, (1 + z // 3) * 2 + c)
            for k in (out_f, 1 - out_f):
                remote(part.at[i, k], from_outer.at[i, k], sent.at[9], o_recv.at[i, k], to).start()

    def stage_r1(i):
        @pl.when(z % 3 != 0)
        def _():
            wait_bytes(from_outer.at[i, mid_f], o_recv.at[i, mid_f])
            summed[i] = (from_outer[i, mid_f].astype(F32) + part[i, mid_f].astype(F32)).astype(BF16)
            remote(summed.at[i], from_mid.at[i], sent.at[9], mid_recv.at[i], (dp, (3 - z) * 2 + c)).start()

    def stage_r2(i):
        @pl.when(z % 3 != 0)
        def _():
            own = 1 - mid_f
            wait_bytes(from_outer.at[i, own], o_recv.at[i, own])
            wait_bytes(from_mid.at[i], mid_recv.at[i])
            value = from_outer[i, own].astype(F32) + part[i, own].astype(F32) + from_mid[i].astype(F32)
            score = jnp.where(own == 0, facts_col[i, :, 2:3], facts_col[i, :, 3:4])
            hidden[i, own] = (jax.nn.silu(value[:, :unit]) * value[:, unit:] * score).astype(BF16)
            held = hidden.at[i, own]
            remote(held, held, sent.at[10], h_recv.at[i, own], (dp, (3 - z) * 2 + c)).start()
            remote(held, held, sent.at[10], h_recv.at[i, own], (dp, (z - 1) * 6 + c)).start()

    def stage_r3(i):
        @pl.when(z % 3 != 0)
        def _():
            held = hidden.at[i, mid_f]
            wait_bytes(held, h_recv.at[i, mid_f])
            remote(held, held, sent.at[10], h_recv.at[i, mid_f], (dp, (z - 1) * 6 + c)).start()

    tile = 256

    def stage_m(i):
        @pl.when(i == 0)
        def _():
            wait_bytes(downs, w_recv.at[2])

        @pl.when(z % 3 == 0)
        def _():
            for k in range(2):
                wait_bytes(hidden.at[i, k], h_recv.at[i, k])

        first = facts_col[i, :, 0:1]
        second = facts_col[i, :, 1:2]
        h_first, h_second = hidden[i, 0].astype(F32), hidden[i, 1].astype(F32)
        for e in range(experts):
            value = jnp.where(first == float(e), h_first, jnp.where(second == float(e), h_second, 0.0))
            masked[:, e * unit : (e + 1) * unit] = value.astype(BF16)
        for n in range(dset // tile):
            at = slice(n * tile, (n + 1) * tile)
            result = lax.dot_general(
                masked[...], downs[at, :], (((1,), (1,)), ((), ())), preferred_element_type=F32
            ).astype(BF16).reshape(n_dp, 2, rows, tile)
            for k in range(2):
                sums[i, k, :, :, at] = result[:, k]
        remote(sums.at[i, 1 - c], from_core.at[i], sent.at[11], core_recv.at[i], (dp, mate)).start()

    def parity(i):
        return (i // n_z + i) % 2

    def stage_o1(i):
        wait_bytes(from_core.at[i], core_recv.at[i])
        value = (sums[i, c].astype(F32) + from_core[i].astype(F32)).astype(BF16)
        added[i] = value.reshape(2, 2, rows, dset)

        @pl.when(parity(i) == 0)
        def _():
            remote(added.at[i, :, 1 - x], from_first.at[i], sent.at[12], first_recv.at[i], (x_dp, me)).start()

        @pl.when(parity(i) == 1)
        def _():
            remote(added.at[i, 1 - y], from_first.at[i], sent.at[12], first_recv.at[i], (y_dp, me)).start()

    def stage_o2(i):
        par = parity(i)
        wait_bytes(from_first.at[i], first_recv.at[i])
        for t in range(2):
            own_y = t + par * (y - t)
            own_x = x + par * (t - x)
            paired[i, t] = (added[i, own_y, own_x].astype(F32) + from_first[i, t].astype(F32)).astype(BF16)
        other = 1 - y + par * (y - x)
        to = (y_dp + par * (x_dp - y_dp), me)
        remote(paired.at[i, other], from_second.at[i], sent.at[13], second_recv.at[i], to).start()

    def stage_o3(i):
        par = parity(i)
        wait_bytes(from_second.at[i], second_recv.at[i])
        own = y + par * (x - y)
        value = paired[i, own].astype(F32) + from_second[i].astype(F32)
        final[i] = (value * gmod_z[...]).astype(BF16)
        j, to = i // n_z, i % n_z

        @pl.when(to == z)
        def _():
            land[j * n_z + z] = final[i]

        @pl.when(to != z)
        def _():
            remote(final.at[i], land.at[j * n_z + z], sent.at[14], out_recv.at[j * n_z + z], (dp, to * 2 + c)).start()

    stages = (
        (0, stage_a), (LAG_B, stage_b), (LAG_C, stage_c), (LAG_G, stage_g), (LAG_R1, stage_r1), (LAG_R2, stage_r2),
        (LAG_R3, stage_r3), (LAG_M, stage_m), (LAG_O1, stage_o1), (LAG_O2, stage_o2), (LAG_O3, stage_o3),
    )

    @pl.loop(0, chunks + LAG_O3)
    def _(t):
        for lag, stage in stages:
            if lag == LAG_B:
                @pl.when(jnp.logical_and(t >= DOWN_AT, t < DOWN_AT + experts))
                def _():
                    send_down(t - DOWN_AT)

            @pl.when(jnp.logical_and(t >= lag, t < chunks + lag))
            def _(lag=lag, stage=stage):
                stage(t - lag)

    for j in range(n_j):
        for t in range(1, n_z):
            i = j * n_z + (z + t) % n_z
            wait_bytes(land.at[i], out_recv.at[i])
    for t in range(n_z):
        for j in range(n_j):
            for d in range(n_dp):
                out_ref[j * rows : (j + 1) * rows, home(t, d) : home(t, d) + wide] = land[
                    j * n_z + t, :, d * wide : (d + 1) * wide
                ]

    for a in range(2):
        wait_bytes(weights.at[:, 0 : (n_spot - 1) * block, 0:unit], sent.at[a])
    wait_bytes(downs.at[0 : (n_spot - 1) * block, :], sent.at[2])
    wait_bytes(pieces.at[0 : n_z - 1], sent.at[3])
    wait_bytes(meta.at[0, 0 : n_dp - 1], sent.at[4])
    wait_bytes(meta.at[0 : 2 * n_z - 1], sent.at[5])
    wait_bytes(grid.at[:, 0:3], sent.at[6])
    wait_bytes(grid.at[:, 0:3], sent.at[7])
    wait_bytes(grid.at[:, 0], sent.at[8])

    @pl.when(z % 3 == 0)
    def _():
        wait_bytes(part, sent.at[9])

    @pl.when(z % 3 != 0)
    def _():
        wait_bytes(summed, sent.at[9])
        wait_bytes(hidden, sent.at[10])
        wait_bytes(hidden.at[:, 0], sent.at[10])

    wait_bytes(from_core, sent.at[11])
    wait_bytes(from_first, sent.at[12])
    wait_bytes(from_second, sent.at[13])
    wait_bytes(final.at[0 : chunks - n_j], sent.at[14])


def shards(
    n_z, rows, tokens, routes, router_weight, shift, scale, gate_mod, gate_weight, up_weight, down_weight
):
    tok_dev, width = tokens.shape
    experts, depth, units = gate_weight.shape
    n_spot = width // (depth * n_z)
    n_dp = n_spot // 2
    dset = n_spot * depth
    unit = units // n_spot
    chunks = n_z * tok_dev // rows
    total = n_spot * rows
    vmem = pl.BlockSpec(memory_space=pltpu.VMEM)
    hbm = pl.BlockSpec(memory_space=pl.ANY)
    dma = pltpu.SemaphoreType.DMA
    return pl.pallas_call(
        kernel,
        out_shape=jax.ShapeDtypeStruct((tok_dev, width), BF16),
        in_specs=[vmem] * 6 + [hbm] * 3,
        out_specs=vmem,
        scratch_shapes=[
            pltpu.VMEM((n_z, tok_dev, dset), BF16),
            pltpu.VMEM((chunks, n_spot, rows, dset), BF16),
            pltpu.VMEM((experts, dset, 2 * unit), BF16),
            pltpu.VMEM((dset, experts * unit), BF16),
            pltpu.VMEM((2 * n_z, n_dp, 8, tok_dev), F32),
            pltpu.VMEM((chunks, total, 8), F32),
            pltpu.VMEM((chunks, 2, total, 2 * unit), BF16),
            pltpu.VMEM((chunks, 2, total, 2 * unit), BF16),
            pltpu.VMEM((chunks, total, 2 * unit), BF16),
            pltpu.VMEM((chunks, total, 2 * unit), BF16),
            pltpu.VMEM((chunks, 2, total, unit), BF16),
            pltpu.VMEM((total, experts * unit), BF16),
            pltpu.VMEM((chunks, 2, n_dp, rows, dset), BF16),
            pltpu.VMEM((chunks, n_dp, rows, dset), BF16),
            pltpu.VMEM((chunks, 2, 2, rows, dset), BF16),
            pltpu.VMEM((chunks, 2, rows, dset), BF16),
            pltpu.VMEM((chunks, 2, rows, dset), BF16),
            pltpu.VMEM((chunks, rows, dset), BF16),
            pltpu.VMEM((chunks, rows, dset), BF16),
            pltpu.VMEM((chunks, rows, dset), BF16),
            pltpu.VMEM((1, dset), F32),
            dma((15,)),
            dma((3,)),
            dma((2,)),
            dma((chunks,)),
            dma((chunks,)),
            dma((chunks,)),
            dma((chunks,)),
            dma((chunks,)),
            dma((chunks, 2)),
            dma((chunks,)),
            dma((chunks, 2)),
            dma((chunks,)),
            dma((chunks,)),
            dma((chunks,)),
            dma((chunks,)),
        ],
        compiler_params=pltpu.CompilerParams(
            collective_id=0, has_side_effects=True, vmem_limit_bytes=65000 * 1024
        ),
    )(tokens, router_weight, routes, shift, scale, gate_mod, gate_weight, up_weight, down_weight)


def choose(mesh):
    n_dp, n_owner = mesh.shape["dp"], mesh.shape["expert"]

    def body(*args):
        tokens, shift, weight = args[0], args[3], args[6]
        n_spot = 2 * n_dp
        fits = n_dp == 4 and n_owner == 8 and shift.shape[0] == 1
        fits = fits and tokens.shape[0] == 128 and tokens.shape[1] == n_dp * n_owner * weight.shape[1]
        fits = fits and weight.shape[1] % 128 == 0 and weight.shape[2] == 128 * n_spot and weight.shape[0] <= 8
        if fits:
            return shards(n_owner // 2, ROWS, *args)
        return shards_plain(*args)

    return body


def solution(mesh):
    in_specs = (
        P(("dp", "expert"), None),
        P(("dp", "expert"), None),
        P(),
        P(),
        P(),
        P(),
        P(None, ("dp", "expert"), None),
        P(None, ("dp", "expert"), None),
        P(None, ("dp", "expert"), None),
    )
    out_specs = P(("dp", "expert"), None)
    return jax.shard_map(
        choose(mesh), mesh=mesh, in_specs=in_specs, out_specs=out_specs, check_vma=False)
```

```python
import functools

import jax
import jax.numpy as jnp
from jax import lax
from jax.experimental import pallas as pl
from jax.experimental.pallas import tpu as pltpu
from jax.sharding import PartitionSpec as P

PIX = 4096


EPS = 1e-06

ROWS = 32
LEAD = 2
LAG_B, LAG_C, LAG_G = 2, 4, 5
LAG_R = 1, 2, 3, 4, 5
LAG_M = 9
LAG_O = 1, 2, 3
DOWN_AT, DOWN_STEP = 5, 1
MULTIPLY_AT, SLOW = 14, 6
TAIL = 13
ORDER = ("a", "b", "down", "c", "g", "ra", "rb", "rc", "rd", "re", "o3", "o2", "o1", "m")
RING, HOLD = 4, 8


def send_back(output):
    return lax.all_to_all(output, "expert", split_axis=0, concat_axis=0, tiled=True)


def shards_plain(
    tokens, routes, router_weight, shift, scale, gate_mod, gate_weight, up_weight, down_weight
):
    tok_dev = tokens.shape[0]
    width = tokens.shape[1]
    experts = router_weight.shape[1]
    n_owner = lax.axis_size("expert")
    local_count = experts // n_owner
    capacity = max(2, 3 * tok_dev // experts)
    first_row = (lax.axis_index("dp") * n_owner + lax.axis_index("expert")) * tok_dev
    image = first_row // PIX
    shift_row = lax.dynamic_slice_in_dim(shift, image, 1, 0)
    scale_row = lax.dynamic_slice_in_dim(scale, image, 1, 0)
    gate_row = lax.dynamic_slice_in_dim(gate_mod, image, 1, 0)
    values = tokens.astype(jnp.float32)
    meansq = jnp.mean(values * values, axis=-1, keepdims=True)
    normed = (values * lax.rsqrt(meansq + EPS) * (1.0 + scale_row) + shift_row).astype(jnp.bfloat16)
    logits = jnp.dot(normed, router_weight, preferred_element_type=jnp.float32)
    onehot = routes[:, :, None] == jnp.arange(experts, dtype=jnp.int32)[None, None, :]
    chosen = jnp.sum(jnp.where(onehot, logits[:, None, :], 0.0), axis=-1)
    score = jax.nn.sigmoid(chosen)
    flat = routes.reshape(-1)
    hot = (flat[:, None] == jnp.arange(experts, dtype=jnp.int32)[None, :]).astype(jnp.int32)
    rank = jnp.cumsum(hot, axis=0) - hot
    slot = jnp.sum(rank * hot, axis=-1)
    position = flat * capacity + slot
    source = (
        jnp.zeros((experts * capacity,), jnp.int32)
        .at[position]
        .set(jnp.arange(2 * tok_dev, dtype=jnp.int32) // 2)
    )
    filled = jnp.zeros((experts * capacity,), jnp.bool_).at[position].set(True)
    outgoing = jnp.where(filled[:, None], normed[source], jnp.zeros((), jnp.bfloat16)).reshape(
        experts, capacity, width
    )
    quarter_gate, quarter_up, quarter_down = (
        lax.all_to_all(gate_weight, "expert", split_axis=0, concat_axis=1, tiled=True),
        lax.all_to_all(up_weight, "expert", split_axis=0, concat_axis=1, tiled=True),
        lax.all_to_all(down_weight, "expert", split_axis=0, concat_axis=1, tiled=True),
    )
    w_gate, w_up, w_down = (
        lax.all_gather(quarter_gate, "dp", axis=1, tiled=True),
        lax.all_gather(quarter_up, "dp", axis=1, tiled=True),
        lax.all_gather(quarter_down, "dp", axis=1, tiled=True),
    )
    received = lax.all_to_all(outgoing, "expert", split_axis=0, concat_axis=0, tiled=True)
    slots = received.shape[1]
    grid = received.reshape(n_owner, local_count, slots, width)
    gate = jnp.einsum("nxcd,xdf->nxcf", grid, w_gate, preferred_element_type=jnp.float32)
    upper = jnp.einsum("nxcd,xdf->nxcf", grid, w_up, preferred_element_type=jnp.float32)
    hidden = (jax.nn.silu(gate) * upper).astype(jnp.bfloat16)
    output = jnp.einsum(
        "nxcf,xdf->nxcd", hidden, w_down, preferred_element_type=jnp.float32
    ).astype(jnp.bfloat16)
    output = output.reshape(n_owner * local_count, slots, width)
    incoming = send_back(output)
    picked = (
        incoming.reshape(experts * capacity, width)[position]
        .astype(jnp.float32)
        .reshape(tok_dev, 2, width)
    )
    branch = jnp.sum(score[:, :, None] * picked, axis=1)
    return (gate_row * branch).astype(jnp.bfloat16)


MESH = pl.DeviceIdType.MESH
F32, BF16 = jnp.float32, jnp.bfloat16


def wait_bytes(ref, sem):
    pltpu.make_async_copy(ref, ref, sem).wait()


def kernel(
    tok_ref, router_ref, routes_ref, shift_ref, scale_ref, gmod_ref, gate_ref, up_ref, down_ref, out_ref,
    pieces, grid, weights, downs, meta, facts_col, part, part_out, passing, hidden, masked,
    sums, sums_out, from_core, added, added_out, from_first, paired, paired_out, from_second, final, land, gmod_z,
    sent, w_recv, m_recv, z_recv, x_recv, y_recv, d_recv, c_recv, pass_recv, h_recv,
    core_recv, first_recv, second_recv, out_recv,
):
    dp, me = lax.axis_index("dp"), lax.axis_index("expert")
    n_z = pieces.shape[0]
    z, c = me // 2, me % 2
    x, y = dp % 2, dp // 2
    x_dp, y_dp, d_dp = dp + 1 - 2 * x, dp + 2 - 4 * y, 3 - dp
    mate = me + 1 - 2 * c
    spot, x_spot, y_spot, d_spot = dp * 2 + c, x_dp * 2 + c, y_dp * 2 + c, d_dp * 2 + c
    tok_dev, width = tok_ref.shape
    experts, depth, units = gate_ref.shape
    chunks, n_spot, rows, dset = grid.shape
    n_j = tok_dev // rows
    block = depth
    unit = units // n_spot
    n_dp = n_spot // 2

    def remote(src, dst, send_sem, recv_sem, to):
        return pltpu.make_async_remote_copy(
            src_ref=src, dst_ref=dst, send_sem=send_sem, recv_sem=recv_sem, device_id=to, device_id_type=MESH
        )

    barrier = pltpu.get_barrier_semaphore()
    for t in range(1, n_spot):
        to = (spot + t) % n_spot
        pl.semaphore_signal(barrier, inc=1, device_id=(to // 2, z * 2 + to % 2), device_id_type=MESH)
    for t in range(1, n_z):
        for k in range(2):
            pl.semaphore_signal(barrier, inc=1, device_id=(dp, ((z + t) % n_z) * 2 + k), device_id_type=MESH)
    pl.semaphore_wait(barrier, n_spot - 1 + 2 * (n_z - 1))

    def own_rows(ref, w):
        return ref.at[:, pl.ds(pl.multiple_of(w * block, block), block), :]

    def send_weight(a):
        ref = (gate_ref, up_ref)[a]
        mine = weights.at[:, pl.ds(pl.multiple_of(spot * block, block), block), a * unit : (a + 1) * unit]

        def source(s):
            return ref.at[:, :, pl.ds(pl.multiple_of(s * unit, unit), unit)]

        pltpu.make_async_copy(source(spot), mine, w_recv.at[a]).start()
        for s in (x_dp * 2 + c, y_dp * 2 + 1 - c, d_dp * 2 + c, y_dp * 2 + c, x_dp * 2 + 1 - c, d_dp * 2 + 1 - c, dp * 2 + 1 - c):
            remote(source(s), mine, sent.at[a], w_recv.at[a], (s // 2, z * 2 + s % 2)).start()

    def send_down(e):
        mine = downs.at[
            pl.ds(pl.multiple_of(spot * block, block), block), pl.ds(pl.multiple_of(e * unit, unit), unit)
        ]

        def source(s):
            return down_ref.at[e, :, pl.ds(pl.multiple_of(s * unit, unit), unit)]

        pltpu.make_async_copy(source(spot), mine, w_recv.at[2]).start()
        for s in (x_dp * 2 + c, y_dp * 2 + 1 - c, d_dp * 2 + c, y_dp * 2 + c, x_dp * 2 + 1 - c, d_dp * 2 + 1 - c, dp * 2 + 1 - c):
            remote(source(s), mine, sent.at[2], w_recv.at[2], (s // 2, z * 2 + s % 2)).start()

    send_weight(0)

    fine = 16
    wide = 2 * block

    def home(z_to, d):
        return (d * n_z + z_to) * wide

    @pl.loop(0, n_j)
    def _(j):
        for b in range(rows // fine):
            at = pl.ds(pl.multiple_of(j * rows + b * fine, fine), fine)
            values = tok_ref[at, :].astype(F32)
            meansq = jnp.mean(values * values, axis=-1, keepdims=True)
            fresh = (values * lax.rsqrt(meansq + EPS) * (1.0 + scale_ref[...]) + shift_ref[...]).astype(BF16)
            for t in range(n_z):
                for d in range(n_dp):
                    pieces[t, at, d * wide : (d + 1) * wide] = fresh[:, home(t, d) : home(t, d) + wide]
        span = pl.ds(pl.multiple_of(j * rows, rows), rows)
        grid[j * n_z + z, spot] = pieces[z, span, :]
        for t in range(1, n_z):
            to = (z + t) % n_z
            remote(
                pieces.at[to, span, :], grid.at[j * n_z + z, spot], sent.at[3], z_recv.at[j * n_z + z], (dp, to * 2 + c)
            ).start()

    logits = jnp.zeros((experts, tok_dev), F32)
    for t in range(n_z):
        for d in range(n_dp):
            logits += lax.dot_general(
                router_ref[:, home(t, d) : home(t, d) + wide], pieces[t, :, d * wide : (d + 1) * wide],
                (((1,), (1,)), ((), ())), preferred_element_type=F32,
            )
    names = lax.broadcasted_iota(jnp.int32, logits.shape, 0)
    facts = [routes_ref[k : k + 1, :].astype(F32) for k in range(2)]
    for k in range(2):
        chosen = jnp.sum(jnp.where(routes_ref[k : k + 1, :] == names, logits, 0.0), axis=0, keepdims=True)
        facts.append(jax.nn.sigmoid(chosen))
    lines = lax.broadcasted_iota(jnp.int32, (8, tok_dev), 0)
    table = jnp.zeros((8, tok_dev), F32)
    for k in range(4):
        table = jnp.where(lines == k, facts[k], table)
    meta[me, dp] = table
    def stage_a(i):
        held = grid.at[i, spot]

        @pl.when(i % n_z != z)
        def _():
            wait_bytes(held, z_recv.at[i])

        remote(held, held, sent.at[6], x_recv.at[i], (x_dp, me)).start()
        remote(held, held, sent.at[6], y_recv.at[i], (y_dp, me)).start()

        @pl.when(i < LEAD)
        def _():
            remote(held, held, sent.at[6], d_recv.at[i], (d_dp, me)).start()

        remote(held, held, sent.at[6], c_recv.at[i], (dp, mate)).start()

    def stage_b(i):
        par = (i // n_z + i) % 2
        wait_bytes(grid.at[i, x_spot], x_recv.at[i])
        wait_bytes(grid.at[i, y_spot], y_recv.at[i])

        @pl.when(i >= LEAD)
        def _():
            relayed = grid.at[i, x_spot + par * (y_spot - x_spot)]
            remote(relayed, relayed, sent.at[7], d_recv.at[i], (y_dp + par * (x_dp - y_dp), me)).start()

        for s in (x_spot, y_spot):
            remote(grid.at[i, s], grid.at[i, s], sent.at[7], c_recv.at[i], (dp, mate)).start()

    def stage_c(i):
        held = grid.at[i, d_spot]
        wait_bytes(held, d_recv.at[i])
        remote(held, held, sent.at[8], c_recv.at[i], (dp, mate)).start()

    total = n_spot * rows
    mid_a, mid_b, end_k = 2 - z, z - 1, z // 3
    end_to, mid_to = 1 + z // 3, 3 - z
    outer = (z - 1) * 3

    def at_end(body):
        pl.when(z % 3 == 0)(body)

    def at_mid(body):
        pl.when(z % 3 != 0)(body)

    halves = [slice(h * (total // 2), (h + 1) * (total // 2)) for h in range(2)]

    def pass_on(i, k, h, to):
        remote(
            part_out.at[i, k, halves[h]], passing.at[i, k, halves[h]], sent.at[9], pass_recv.at[i, k, h],
            (dp, to * 2 + c),
        ).start()

    def give(i, k, h, to):
        held = hidden.at[i, k, halves[h]]
        remote(held, held, sent.at[10], h_recv.at[i, k, h], (dp, to * 2 + c)).start()

    def take(i, k, h):
        wait_bytes(hidden.at[i, k, halves[h]], h_recv.at[i, k, h])

    def stage_g(i):
        @pl.when(i == 0)
        def _():
            for a in range(2):
                wait_bytes(weights.at[:, :, a * unit : (a + 1) * unit], w_recv.at[a])

        wait_bytes(grid.at[i, pl.ds(0, n_dp)], c_recv.at[i])
        block_in = grid[i].reshape(total, dset)
        first = facts_col[i, :, 0:1]
        second = facts_col[i, :, 1:2]
        picked = [jnp.zeros((total, 2 * unit), F32)] * 2
        for e in range(experts):
            result = jnp.dot(block_in, weights[e], preferred_element_type=F32)
            picked = [jnp.where(who == float(e), result, old) for who, old in zip((first, second), picked)]
        for k in range(2):
            part[i % HOLD, k] = picked[k]

        @at_end
        def _():
            part_out[i, 1 - end_k] = part[i % HOLD, 1 - end_k].astype(BF16)
            for h in range(2):
                pass_on(i, 1 - end_k, h, end_to)

    def add_on(i, k, to):
        for h in range(2):
            at = halves[h]
            wait_bytes(passing.at[i, k, at], pass_recv.at[i, k, h])
            part_out[i, k, at] = (passing[i, k, at].astype(F32) + part[i % HOLD, k, at]).astype(BF16)
            pass_on(i, k, h, to)

    def stage_ra(i):
        at_mid(lambda: add_on(i, mid_a, mid_to))

    def stage_rb(i):
        at_mid(lambda: add_on(i, mid_b, outer))

    def stage_rc(i):
        @at_end
        def _():
            for h in range(2):
                at = halves[h]
                wait_bytes(passing.at[i, end_k, at], pass_recv.at[i, end_k, h])
                value = passing[i, end_k, at].astype(F32) + part[i % HOLD, end_k, at]
                score = jnp.where(end_k == 0, facts_col[i, at, 2:3], facts_col[i, at, 3:4])
                hidden[i, end_k, at] = (jax.nn.silu(value[:, :unit]) * value[:, unit:] * score).astype(BF16)
                give(i, end_k, h, end_to)

                @pl.when(i >= TAIL)
                def _():
                    give(i, end_k, h, 3 - end_to)
                    give(i, end_k, h, 3 - z)

    def relay_hidden(i, k, to):
        for h in range(2):
            take(i, k, h)
            give(i, k, h, to)

    def stage_rd(i):
        at_mid(lambda: relay_hidden(i, mid_b, mid_to))

    def stage_re(i):
        at_mid(lambda: relay_hidden(i, mid_a, outer))

    tile = 256

    def stage_m(i):
        @pl.when(i == 0)
        def _():
            wait_bytes(downs, w_recv.at[2])

        @pl.when(z % 3 == 0)
        def _():
            for h in range(2):
                take(i, 1 - end_k, h)

        @pl.when(jnp.logical_and(z % 3 != 0, i >= TAIL))
        def _():
            for k in range(2):
                for h in range(2):
                    take(i, k, h)

        first = facts_col[i, :, 0:1]
        second = facts_col[i, :, 1:2]
        h_first, h_second = hidden[i, 0].astype(F32), hidden[i, 1].astype(F32)
        for e in range(experts):
            value = jnp.where(first == float(e), h_first, jnp.where(second == float(e), h_second, 0.0))
            masked[:, e * unit : (e + 1) * unit] = value.astype(BF16)
        for n in range(dset // tile):
            at = slice(n * tile, (n + 1) * tile)
            result = lax.dot_general(
                masked[...], downs[at, :], (((1,), (1,)), ((), ())), preferred_element_type=F32
            ).reshape(n_dp, 2, rows, tile)
            sums[i % RING, :, :, at] = jnp.where(c == 0, result[:, 0], result[:, 1])
            sums_out[i, :, :, at] = jnp.where(c == 0, result[:, 1], result[:, 0]).astype(BF16)
        remote(sums_out.at[i], from_core.at[i], sent.at[11], core_recv.at[i], (dp, mate)).start()

    def parity(i):
        return (i // n_z + i) % 2

    def stage_o1(i):
        par = parity(i)
        wait_bytes(from_core.at[i], core_recv.at[i])
        for t in range(2):
            own = (t + par * (y - t)) * 2 + x + par * (t - x)
            away = (t + par * (1 - y - t)) * 2 + 1 - x + par * (t - 1 + x)
            added_out[i, t] = (sums[i % RING, away] + from_core[i, away].astype(F32)).astype(BF16)
            added[i % RING, t] = sums[i % RING, own] + from_core[i, own].astype(F32)
        keep = y + par * (x - y)
        for s in (1 - keep, keep):
            remote(
                added_out.at[i, s], from_first.at[i, s], sent.at[12], first_recv.at[i, s],
                (x_dp + par * (y_dp - x_dp), me),
            ).start()

    def stage_o2(i):
        par = parity(i)
        own = y + par * (x - y)
        wait_bytes(from_first.at[i, 1 - own], first_recv.at[i, 1 - own])
        paired_out[i] = (added[i % RING, 1 - own] + from_first[i, 1 - own].astype(F32)).astype(BF16)
        remote(
            paired_out.at[i], from_second.at[i], sent.at[13], second_recv.at[i], (y_dp + par * (x_dp - y_dp), me)
        ).start()
        wait_bytes(from_first.at[i, own], first_recv.at[i, own])
        paired[i % RING] = added[i % RING, own] + from_first[i, own].astype(F32)

    def stage_o3(i):
        wait_bytes(from_second.at[i], second_recv.at[i])
        value = paired[i % RING] + from_second[i].astype(F32)
        final[i] = (value * gmod_z[...]).astype(BF16)
        j, to = i // n_z, i % n_z

        @pl.when(to == z)
        def _():
            land[j * n_z + z] = final[i]

        @pl.when(to != z)
        def _():
            remote(final.at[i], land.at[j * n_z + z], sent.at[14], out_recv.at[j * n_z + z], (dp, to * 2 + c)).start()

    def even(t, lag, stage, count=chunks):
        @pl.when(jnp.logical_and(t >= lag, t < count + lag))
        def _():
            stage(t - lag)

    def paced(t, shift, stage):
        start, twice, late = MULTIPLY_AT + shift, MULTIPLY_AT + SLOW + shift, LAG_M + shift
        single = twice + MULTIPLY_AT - LAG_M

        @pl.when(jnp.logical_and(t >= start, t < twice))
        def _():
            stage(t - start)

        @pl.when(jnp.logical_and(t >= twice, t < single))
        def _():
            @pl.loop(0, 2)
            def _(s):
                stage(SLOW + 2 * (t - twice) + s)

        @pl.when(jnp.logical_and(t >= single, t < chunks + late))
        def _():
            stage(t - late)

    for i in range(LEAD):
        stage_a(i)
    for to in (x_dp, y_dp, d_dp):
        remote(meta.at[me, dp], meta.at[me, dp], sent.at[4], m_recv.at[0], (to, me)).start()
    send_weight(1)
    for d in range(n_dp):
        gmod_z[:, d * wide : (d + 1) * wide] = gmod_ref[
            :, pl.ds(pl.multiple_of((d * n_z + z) * wide, wide), wide)
        ]
    wait_bytes(meta.at[me, pl.ds(0, n_dp - 1)], m_recv.at[0])
    for t in range(1, 2 * n_z):
        remote(meta.at[me], meta.at[me], sent.at[5], m_recv.at[1], (dp, (me + t) % (2 * n_z))).start()
    wait_bytes(meta.at[pl.ds(0, 2 * n_z - 1)], m_recv.at[1])

    @pl.loop(0, 2 * n_z)
    def _(e):
        for d in range(n_dp):
            column = meta[e, d].T
            for j in range(n_j):
                at = pl.ds(pl.multiple_of((d * 2 + e % 2) * rows, rows), rows)
                facts_col[j * n_z + e // 2, at, :] = column[j * rows : (j + 1) * rows, :]

    def send_ahead(t):
        @pl.when(jnp.logical_and(t >= LEAD, t < chunks))
        def _():
            stage_a(t)

    def send_downs(t):
        ahead = t - DOWN_AT

        @pl.when(jnp.logical_and(ahead >= 0, jnp.logical_and(ahead < experts * DOWN_STEP, ahead % DOWN_STEP == 0)))
        def _():
            send_down(ahead // DOWN_STEP)

    steps = {
        "a": send_ahead,
        "b": lambda t: even(t, LAG_B, stage_b),
        "down": send_downs,
        "c": lambda t: even(t, LAG_C, stage_c),
        "g": lambda t: even(t, LAG_G, stage_g),
        "ra": lambda t: even(t, LAG_G + LAG_R[0], stage_ra),
        "rb": lambda t: even(t, LAG_G + LAG_R[1], stage_rb),
        "rc": lambda t: even(t, LAG_G + LAG_R[2], stage_rc),
        "rd": lambda t: even(t, LAG_G + LAG_R[3], stage_rd, TAIL),
        "re": lambda t: even(t, LAG_G + LAG_R[4], stage_re, TAIL),
        "m": lambda t: paced(t, 0, stage_m),
        "o1": lambda t: paced(t, LAG_O[0], stage_o1),
        "o2": lambda t: paced(t, LAG_O[1], stage_o2),
        "o3": lambda t: paced(t, LAG_O[2], stage_o3),
    }

    @pl.loop(LAG_B, chunks + LAG_M + LAG_O[2])
    def _(t):
        for name in ORDER:
            steps[name](t)

    for j in range(n_j):
        for t in range(1, n_z):
            i = j * n_z + (z + t) % n_z
            wait_bytes(land.at[i], out_recv.at[i])
    for t in range(n_z):
        for j in range(n_j):
            for d in range(n_dp):
                out_ref[j * rows : (j + 1) * rows, home(t, d) : home(t, d) + wide] = land[
                    j * n_z + t, :, d * wide : (d + 1) * wide
                ]

    for a in range(2):
        wait_bytes(weights.at[:, 0 : (n_spot - 1) * block, 0:unit], sent.at[a])
    wait_bytes(downs.at[0 : (n_spot - 1) * block, :], sent.at[2])
    wait_bytes(pieces.at[0 : n_z - 1], sent.at[3])
    wait_bytes(meta.at[0, 0 : n_dp - 1], sent.at[4])
    wait_bytes(meta.at[0 : 2 * n_z - 1], sent.at[5])
    wait_bytes(grid.at[:, 0:3], sent.at[6])
    wait_bytes(grid.at[0:LEAD, 0], sent.at[6])
    wait_bytes(grid.at[:, 0:2], sent.at[7])
    wait_bytes(grid.at[LEAD:chunks, 0], sent.at[7])
    wait_bytes(grid.at[:, 0], sent.at[8])

    @at_end
    def _():
        wait_bytes(part_out.at[:, 0], sent.at[9])
        wait_bytes(hidden.at[:, 0], sent.at[10])
        wait_bytes(hidden.at[TAIL:chunks], sent.at[10])

    @at_mid
    def _():
        wait_bytes(part_out, sent.at[9])
        wait_bytes(hidden.at[0:TAIL], sent.at[10])

    wait_bytes(from_core, sent.at[11])
    wait_bytes(from_first, sent.at[12])
    wait_bytes(from_second, sent.at[13])
    wait_bytes(final.at[0 : chunks - n_j], sent.at[14])


def shards(
    n_z, rows, tokens, routes, router_weight, shift, scale, gate_mod, gate_weight, up_weight, down_weight
):
    tok_dev, width = tokens.shape
    experts, depth, units = gate_weight.shape
    n_spot = width // (depth * n_z)
    n_dp = n_spot // 2
    dset = n_spot * depth
    unit = units // n_spot
    chunks = n_z * tok_dev // rows
    total = n_spot * rows
    vmem = pl.BlockSpec(memory_space=pltpu.VMEM)
    hbm = pl.BlockSpec(memory_space=pl.ANY)
    dma = pltpu.SemaphoreType.DMA
    return pl.pallas_call(
        kernel,
        out_shape=jax.ShapeDtypeStruct((tok_dev, width), BF16),
        in_specs=[vmem] * 6 + [hbm] * 3,
        out_specs=vmem,
        scratch_shapes=[
            pltpu.VMEM((n_z, tok_dev, dset), BF16),
            pltpu.VMEM((chunks, n_spot, rows, dset), BF16),
            pltpu.VMEM((experts, dset, 2 * unit), BF16),
            pltpu.VMEM((dset, experts * unit), BF16),
            pltpu.VMEM((2 * n_z, n_dp, 8, tok_dev), F32),
            pltpu.VMEM((chunks, total, 8), F32),
            pltpu.VMEM((HOLD, 2, total, 2 * unit), F32),
            pltpu.VMEM((chunks, 2, total, 2 * unit), BF16),
            pltpu.VMEM((chunks, 2, total, 2 * unit), BF16),
            pltpu.VMEM((chunks, 2, total, unit), BF16),
            pltpu.VMEM((total, experts * unit), BF16),
            pltpu.VMEM((RING, n_dp, rows, dset), F32),
            pltpu.VMEM((chunks, n_dp, rows, dset), BF16),
            pltpu.VMEM((chunks, n_dp, rows, dset), BF16),
            pltpu.VMEM((RING, 2, rows, dset), F32),
            pltpu.VMEM((chunks, 2, rows, dset), BF16),
            pltpu.VMEM((chunks, 2, rows, dset), BF16),
            pltpu.VMEM((RING, rows, dset), F32),
            pltpu.VMEM((chunks, rows, dset), BF16),
            pltpu.VMEM((chunks, rows, dset), BF16),
            pltpu.VMEM((chunks, rows, dset), BF16),
            pltpu.VMEM((chunks, rows, dset), BF16),
            pltpu.VMEM((1, dset), F32),
            dma((15,)),
            dma((3,)),
            dma((2,)),
            dma((chunks,)),
            dma((chunks,)),
            dma((chunks,)),
            dma((chunks,)),
            dma((chunks,)),
            dma((chunks, 2, 2)),
            dma((chunks, 2, 2)),
            dma((chunks,)),
            dma((chunks, 2)),
            dma((chunks,)),
            dma((chunks,)),
        ],
        compiler_params=pltpu.CompilerParams(
            collective_id=0, has_side_effects=True, vmem_limit_bytes=65000 * 1024
        ),
    )(tokens, router_weight.T, routes.T, shift, scale, gate_mod, gate_weight, up_weight, down_weight)


def choose(mesh):
    n_dp, n_owner = mesh.shape["dp"], mesh.shape["expert"]

    def body(*args):
        tokens, shift, weight = args[0], args[3], args[6]
        n_spot = 2 * n_dp
        fits = n_dp == 4 and n_owner == 8 and shift.shape[0] == 1
        fits = fits and tokens.shape[0] == 128 and tokens.shape[1] == n_dp * n_owner * weight.shape[1]
        fits = fits and weight.shape[1] % 128 == 0 and weight.shape[2] == 128 * n_spot and weight.shape[0] <= 8
        if fits:
            return shards(n_owner // 2, ROWS, *args)
        return shards_plain(*args)

    return body


def solution(mesh):
    in_specs = (
        P(("dp", "expert"), None),
        P(("dp", "expert"), None),
        P(),
        P(),
        P(),
        P(),
        P(None, ("dp", "expert"), None),
        P(None, ("dp", "expert"), None),
        P(None, ("dp", "expert"), None),
    )
    out_specs = P(("dp", "expert"), None)
    return jax.shard_map(
        choose(mesh), mesh=mesh, in_specs=in_specs, out_specs=out_specs, check_vma=False)
```

```python
import functools

import jax
import jax.numpy as jnp
from jax import lax
from jax.experimental import pallas as pl
from jax.experimental.pallas import tpu as pltpu
from jax.sharding import PartitionSpec as P

PIX = 4096


EPS = 1e-06

ROWS = 32
LEAD = 2
LAG_B, LAG_C, LAG_G = 2, 4, 5
LAG_R = 1, 2, 3, 4, 5
LAG_M = 9
LAG_O = 1, 2, 3
DOWN_AT, DOWN_STEP = 5, 1
MULTIPLY_AT, SLOW = 14, 6
TAIL = 13
TILE = 256
ORDER = ("a", "b", "down", "c", "g", "ra", "rb", "rc", "rd", "re", "o3", "o2", "o1", "m")
RING, HOLD = 4, 8


def send_back(output):
    return lax.all_to_all(output, "expert", split_axis=0, concat_axis=0, tiled=True)


def shards_plain(
    tokens, routes, router_weight, shift, scale, gate_mod, gate_weight, up_weight, down_weight
):
    tok_dev = tokens.shape[0]
    width = tokens.shape[1]
    experts = router_weight.shape[1]
    n_owner = lax.axis_size("expert")
    local_count = experts // n_owner
    capacity = max(2, 3 * tok_dev // experts)
    first_row = (lax.axis_index("dp") * n_owner + lax.axis_index("expert")) * tok_dev
    image = first_row // PIX
    shift_row = lax.dynamic_slice_in_dim(shift, image, 1, 0)
    scale_row = lax.dynamic_slice_in_dim(scale, image, 1, 0)
    gate_row = lax.dynamic_slice_in_dim(gate_mod, image, 1, 0)
    values = tokens.astype(jnp.float32)
    meansq = jnp.mean(values * values, axis=-1, keepdims=True)
    normed = (values * lax.rsqrt(meansq + EPS) * (1.0 + scale_row) + shift_row).astype(jnp.bfloat16)
    logits = jnp.dot(normed, router_weight, preferred_element_type=jnp.float32)
    onehot = routes[:, :, None] == jnp.arange(experts, dtype=jnp.int32)[None, None, :]
    chosen = jnp.sum(jnp.where(onehot, logits[:, None, :], 0.0), axis=-1)
    score = jax.nn.sigmoid(chosen)
    flat = routes.reshape(-1)
    hot = (flat[:, None] == jnp.arange(experts, dtype=jnp.int32)[None, :]).astype(jnp.int32)
    rank = jnp.cumsum(hot, axis=0) - hot
    slot = jnp.sum(rank * hot, axis=-1)
    position = flat * capacity + slot
    source = (
        jnp.zeros((experts * capacity,), jnp.int32)
        .at[position]
        .set(jnp.arange(2 * tok_dev, dtype=jnp.int32) // 2)
    )
    filled = jnp.zeros((experts * capacity,), jnp.bool_).at[position].set(True)
    outgoing = jnp.where(filled[:, None], normed[source], jnp.zeros((), jnp.bfloat16)).reshape(
        experts, capacity, width
    )
    quarter_gate, quarter_up, quarter_down = (
        lax.all_to_all(gate_weight, "expert", split_axis=0, concat_axis=1, tiled=True),
        lax.all_to_all(up_weight, "expert", split_axis=0, concat_axis=1, tiled=True),
        lax.all_to_all(down_weight, "expert", split_axis=0, concat_axis=1, tiled=True),
    )
    w_gate, w_up, w_down = (
        lax.all_gather(quarter_gate, "dp", axis=1, tiled=True),
        lax.all_gather(quarter_up, "dp", axis=1, tiled=True),
        lax.all_gather(quarter_down, "dp", axis=1, tiled=True),
    )
    received = lax.all_to_all(outgoing, "expert", split_axis=0, concat_axis=0, tiled=True)
    slots = received.shape[1]
    grid = received.reshape(n_owner, local_count, slots, width)
    gate = jnp.einsum("nxcd,xdf->nxcf", grid, w_gate, preferred_element_type=jnp.float32)
    upper = jnp.einsum("nxcd,xdf->nxcf", grid, w_up, preferred_element_type=jnp.float32)
    hidden = (jax.nn.silu(gate) * upper).astype(jnp.bfloat16)
    output = jnp.einsum(
        "nxcf,xdf->nxcd", hidden, w_down, preferred_element_type=jnp.float32
    ).astype(jnp.bfloat16)
    output = output.reshape(n_owner * local_count, slots, width)
    incoming = send_back(output)
    picked = (
        incoming.reshape(experts * capacity, width)[position]
        .astype(jnp.float32)
        .reshape(tok_dev, 2, width)
    )
    branch = jnp.sum(score[:, :, None] * picked, axis=1)
    return (gate_row * branch).astype(jnp.bfloat16)


MESH = pl.DeviceIdType.MESH
F32, BF16 = jnp.float32, jnp.bfloat16


def wait_bytes(ref, sem):
    pltpu.make_async_copy(ref, ref, sem).wait()


def kernel(
    tok_ref, router_ref, routes_ref, shift_ref, scale_ref, gmod_ref, gate_ref, up_ref, down_ref, out_ref,
    pieces, grid, weights, downs, meta, facts_col, part, part_out, passing, hidden, masked,
    sums, sums_out, from_core, added, added_out, from_first, paired, paired_out, from_second, final, land, gmod_z,
    sent, w_recv, m_recv, z_recv, x_recv, y_recv, d_recv, c_recv, pass_recv, h_recv,
    core_recv, first_recv, second_recv, out_recv,
):
    dp, me = lax.axis_index("dp"), lax.axis_index("expert")
    n_z = pieces.shape[0]
    z, c = me // 2, me % 2
    x, y = dp % 2, dp // 2
    x_dp, y_dp, d_dp = dp + 1 - 2 * x, dp + 2 - 4 * y, 3 - dp
    mate = me + 1 - 2 * c
    spot, x_spot, y_spot, d_spot = dp * 2 + c, x_dp * 2 + c, y_dp * 2 + c, d_dp * 2 + c
    tok_dev, width = tok_ref.shape
    experts, depth, units = gate_ref.shape
    chunks, n_spot, rows, dset = grid.shape
    n_j = tok_dev // rows
    block = depth
    unit = units // n_spot
    n_dp = n_spot // 2

    def remote(src, dst, send_sem, recv_sem, to):
        return pltpu.make_async_remote_copy(
            src_ref=src, dst_ref=dst, send_sem=send_sem, recv_sem=recv_sem, device_id=to, device_id_type=MESH
        )

    barrier = pltpu.get_barrier_semaphore()
    for t in range(1, n_spot):
        to = (spot + t) % n_spot
        pl.semaphore_signal(barrier, inc=1, device_id=(to // 2, z * 2 + to % 2), device_id_type=MESH)
    for t in range(1, n_z):
        for k in range(2):
            pl.semaphore_signal(barrier, inc=1, device_id=(dp, ((z + t) % n_z) * 2 + k), device_id_type=MESH)
    pl.semaphore_wait(barrier, n_spot - 1 + 2 * (n_z - 1))

    def own_rows(ref, w):
        return ref.at[:, pl.ds(pl.multiple_of(w * block, block), block), :]

    def send_weight(a):
        ref = (gate_ref, up_ref)[a]
        mine = weights.at[:, pl.ds(pl.multiple_of(spot * block, block), block), a * unit : (a + 1) * unit]

        def source(s):
            return ref.at[:, :, pl.ds(pl.multiple_of(s * unit, unit), unit)]

        pltpu.make_async_copy(source(spot), mine, w_recv.at[a]).start()
        for s in (x_dp * 2 + c, y_dp * 2 + 1 - c, d_dp * 2 + c, y_dp * 2 + c, x_dp * 2 + 1 - c, d_dp * 2 + 1 - c, dp * 2 + 1 - c):
            remote(source(s), mine, sent.at[a], w_recv.at[a], (s // 2, z * 2 + s % 2)).start()

    def send_down(e):
        mine = downs.at[
            pl.ds(pl.multiple_of(spot * block, block), block), pl.ds(pl.multiple_of(e * unit, unit), unit)
        ]

        def source(s):
            return down_ref.at[e, :, pl.ds(pl.multiple_of(s * unit, unit), unit)]

        pltpu.make_async_copy(source(spot), mine, w_recv.at[2]).start()
        for s in (x_dp * 2 + c, y_dp * 2 + 1 - c, d_dp * 2 + c, y_dp * 2 + c, x_dp * 2 + 1 - c, d_dp * 2 + 1 - c, dp * 2 + 1 - c):
            remote(source(s), mine, sent.at[2], w_recv.at[2], (s // 2, z * 2 + s % 2)).start()

    send_weight(0)

    fine = 16
    wide = 2 * block

    def home(z_to, d):
        return (d * n_z + z_to) * wide

    @pl.loop(0, n_j)
    def _(j):
        for b in range(rows // fine):
            at = pl.ds(pl.multiple_of(j * rows + b * fine, fine), fine)
            values = tok_ref[at, :].astype(F32)
            meansq = jnp.mean(values * values, axis=-1, keepdims=True)
            fresh = (values * lax.rsqrt(meansq + EPS) * (1.0 + scale_ref[...]) + shift_ref[...]).astype(BF16)
            for t in range(n_z):
                for d in range(n_dp):
                    pieces[t, at, d * wide : (d + 1) * wide] = fresh[:, home(t, d) : home(t, d) + wide]
        span = pl.ds(pl.multiple_of(j * rows, rows), rows)
        grid[j * n_z + z, spot] = pieces[z, span, :]
        for t in range(1, n_z):
            to = (z + t) % n_z
            remote(
                pieces.at[to, span, :], grid.at[j * n_z + z, spot], sent.at[3], z_recv.at[j * n_z + z], (dp, to * 2 + c)
            ).start()

    logits = jnp.zeros((experts, tok_dev), F32)
    for t in range(n_z):
        for d in range(n_dp):
            logits += lax.dot_general(
                router_ref[:, home(t, d) : home(t, d) + wide], pieces[t, :, d * wide : (d + 1) * wide],
                (((1,), (1,)), ((), ())), preferred_element_type=F32,
            )
    names = lax.broadcasted_iota(jnp.int32, logits.shape, 0)
    facts = [routes_ref[k : k + 1, :].astype(F32) for k in range(2)]
    for k in range(2):
        chosen = jnp.sum(jnp.where(routes_ref[k : k + 1, :] == names, logits, 0.0), axis=0, keepdims=True)
        facts.append(jax.nn.sigmoid(chosen))
    lines = lax.broadcasted_iota(jnp.int32, (8, tok_dev), 0)
    table = jnp.zeros((8, tok_dev), F32)
    for k in range(4):
        table = jnp.where(lines == k, facts[k], table)
    meta[me, dp] = table
    def stage_a(i):
        held = grid.at[i, spot]

        @pl.when(i % n_z != z)
        def _():
            wait_bytes(held, z_recv.at[i])

        remote(held, held, sent.at[6], x_recv.at[i], (x_dp, me)).start()
        remote(held, held, sent.at[6], y_recv.at[i], (y_dp, me)).start()

        @pl.when(i < LEAD)
        def _():
            remote(held, held, sent.at[6], d_recv.at[i], (d_dp, me)).start()

        remote(held, held, sent.at[6], c_recv.at[i], (dp, mate)).start()

    def stage_b(i):
        par = (i // n_z + i) % 2
        wait_bytes(grid.at[i, x_spot], x_recv.at[i])
        wait_bytes(grid.at[i, y_spot], y_recv.at[i])

        @pl.when(i >= LEAD)
        def _():
            relayed = grid.at[i, x_spot + par * (y_spot - x_spot)]
            remote(relayed, relayed, sent.at[7], d_recv.at[i], (y_dp + par * (x_dp - y_dp), me)).start()

        for s in (x_spot, y_spot):
            remote(grid.at[i, s], grid.at[i, s], sent.at[7], c_recv.at[i], (dp, mate)).start()

    def stage_c(i):
        held = grid.at[i, d_spot]
        wait_bytes(held, d_recv.at[i])
        remote(held, held, sent.at[8], c_recv.at[i], (dp, mate)).start()

    total = n_spot * rows
    mid_a, mid_b, end_k = 2 - z, z - 1, z // 3
    end_to, mid_to = 1 + z // 3, 3 - z
    outer = (z - 1) * 3

    def at_end(body):
        pl.when(z % 3 == 0)(body)

    def at_mid(body):
        pl.when(z % 3 != 0)(body)

    halves = [slice(h * (total // 2), (h + 1) * (total // 2)) for h in range(2)]

    def pass_on(i, k, h, to):
        remote(
            part_out.at[i, k, halves[h]], passing.at[i, k, halves[h]], sent.at[9], pass_recv.at[i, k, h],
            (dp, to * 2 + c),
        ).start()

    def give(i, k, h, to):
        held = hidden.at[i, k, halves[h]]
        remote(held, held, sent.at[10], h_recv.at[i, k, h], (dp, to * 2 + c)).start()

    def take(i, k, h):
        wait_bytes(hidden.at[i, k, halves[h]], h_recv.at[i, k, h])

    def stage_g(i):
        @pl.when(i == 0)
        def _():
            for a in range(2):
                wait_bytes(weights.at[:, :, a * unit : (a + 1) * unit], w_recv.at[a])

        wait_bytes(grid.at[i, pl.ds(0, n_dp)], c_recv.at[i])
        block_in = grid[i].reshape(total, dset)
        first = facts_col[i, :, 0:1]
        second = facts_col[i, :, 1:2]
        picked = [jnp.zeros((total, 2 * unit), F32)] * 2
        for e in range(experts):
            result = jnp.dot(block_in, weights[e], preferred_element_type=F32)
            picked = [jnp.where(who == float(e), result, old) for who, old in zip((first, second), picked)]
        for k in range(2):
            part[i % HOLD, k] = picked[k]

        @at_end
        def _():
            part_out[i, 1 - end_k] = part[i % HOLD, 1 - end_k].astype(BF16)
            for h in range(2):
                pass_on(i, 1 - end_k, h, end_to)

    def add_on(i, k, to):
        for h in range(2):
            at = halves[h]
            wait_bytes(passing.at[i, k, at], pass_recv.at[i, k, h])
            part_out[i, k, at] = (passing[i, k, at].astype(F32) + part[i % HOLD, k, at]).astype(BF16)
            pass_on(i, k, h, to)

    def stage_ra(i):
        at_mid(lambda: add_on(i, mid_a, mid_to))

    def stage_rb(i):
        at_mid(lambda: add_on(i, mid_b, outer))

    def stage_rc(i):
        @at_end
        def _():
            for h in range(2):
                at = halves[h]
                wait_bytes(passing.at[i, end_k, at], pass_recv.at[i, end_k, h])
                value = passing[i, end_k, at].astype(F32) + part[i % HOLD, end_k, at]
                score = jnp.where(end_k == 0, facts_col[i, at, 2:3], facts_col[i, at, 3:4])
                hidden[i, end_k, at] = (jax.nn.silu(value[:, :unit]) * value[:, unit:] * score).astype(BF16)
                give(i, end_k, h, end_to)

                @pl.when(i >= TAIL)
                def _():
                    give(i, end_k, h, 3 - end_to)
                    give(i, end_k, h, 3 - z)

    def relay_hidden(i, k, to):
        for h in range(2):
            take(i, k, h)
            give(i, k, h, to)

    def stage_rd(i):
        at_mid(lambda: relay_hidden(i, mid_b, mid_to))

    def stage_re(i):
        at_mid(lambda: relay_hidden(i, mid_a, outer))

    tile = TILE

    def stage_m(i):
        @pl.when(i == 0)
        def _():
            wait_bytes(downs, w_recv.at[2])

        @pl.when(z % 3 == 0)
        def _():
            for h in range(2):
                take(i, 1 - end_k, h)

        @pl.when(jnp.logical_and(z % 3 != 0, i >= TAIL))
        def _():
            for k in range(2):
                for h in range(2):
                    take(i, k, h)

        first = facts_col[i, :, 0:1]
        second = facts_col[i, :, 1:2]
        h_first, h_second = hidden[i, 0].astype(F32), hidden[i, 1].astype(F32)
        for e in range(experts):
            value = jnp.where(first == float(e), h_first, jnp.where(second == float(e), h_second, 0.0))
            masked[:, e * unit : (e + 1) * unit] = value.astype(BF16)
        for n in range(dset // tile):
            at = slice(n * tile, (n + 1) * tile)
            result = lax.dot_general(
                masked[...], downs[at, :], (((1,), (1,)), ((), ())), preferred_element_type=F32
            ).reshape(n_dp, 2, rows, tile)
            sums[i % RING, :, :, at] = jnp.where(c == 0, result[:, 0], result[:, 1])
            sums_out[i, :, :, at] = jnp.where(c == 0, result[:, 1], result[:, 0]).astype(BF16)
        remote(sums_out.at[i], from_core.at[i], sent.at[11], core_recv.at[i], (dp, mate)).start()

    def parity(i):
        return (i // n_z + i) % 2

    def stage_o1(i):
        par = parity(i)
        wait_bytes(from_core.at[i], core_recv.at[i])
        for t in range(2):
            own = (t + par * (y - t)) * 2 + x + par * (t - x)
            away = (t + par * (1 - y - t)) * 2 + 1 - x + par * (t - 1 + x)
            added_out[i, t] = (sums[i % RING, away] + from_core[i, away].astype(F32)).astype(BF16)
            added[i % RING, t] = sums[i % RING, own] + from_core[i, own].astype(F32)
        keep = y + par * (x - y)
        for s in (1 - keep, keep):
            remote(
                added_out.at[i, s], from_first.at[i, s], sent.at[12], first_recv.at[i, s],
                (x_dp + par * (y_dp - x_dp), me),
            ).start()

    def stage_o2(i):
        par = parity(i)
        own = y + par * (x - y)
        wait_bytes(from_first.at[i, 1 - own], first_recv.at[i, 1 - own])
        paired_out[i] = (added[i % RING, 1 - own] + from_first[i, 1 - own].astype(F32)).astype(BF16)
        remote(
            paired_out.at[i], from_second.at[i], sent.at[13], second_recv.at[i], (y_dp + par * (x_dp - y_dp), me)
        ).start()
        wait_bytes(from_first.at[i, own], first_recv.at[i, own])
        paired[i % RING] = added[i % RING, own] + from_first[i, own].astype(F32)

    def stage_o3(i):
        wait_bytes(from_second.at[i], second_recv.at[i])
        value = paired[i % RING] + from_second[i].astype(F32)
        final[i] = (value * gmod_z[...]).astype(BF16)
        j, to = i // n_z, i % n_z

        @pl.when(to == z)
        def _():
            land[j * n_z + z] = final[i]

        @pl.when(to != z)
        def _():
            remote(final.at[i], land.at[j * n_z + z], sent.at[14], out_recv.at[j * n_z + z], (dp, to * 2 + c)).start()

    def even(t, lag, stage, count=chunks):
        @pl.when(jnp.logical_and(t >= lag, t < count + lag))
        def _():
            stage(t - lag)

    def paced(t, shift, stage):
        start, twice, late = MULTIPLY_AT + shift, MULTIPLY_AT + SLOW + shift, LAG_M + shift
        single = twice + MULTIPLY_AT - LAG_M

        @pl.when(jnp.logical_and(t >= start, t < twice))
        def _():
            stage(t - start)

        @pl.when(jnp.logical_and(t >= twice, t < single))
        def _():
            @pl.loop(0, 2)
            def _(s):
                stage(SLOW + 2 * (t - twice) + s)

        @pl.when(jnp.logical_and(t >= single, t < chunks + late))
        def _():
            stage(t - late)

    for i in range(LEAD):
        stage_a(i)
    for to in (x_dp, y_dp, d_dp):
        remote(meta.at[me, dp], meta.at[me, dp], sent.at[4], m_recv.at[0], (to, me)).start()
    send_weight(1)
    for d in range(n_dp):
        gmod_z[:, d * wide : (d + 1) * wide] = gmod_ref[
            :, pl.ds(pl.multiple_of((d * n_z + z) * wide, wide), wide)
        ]
    wait_bytes(meta.at[me, pl.ds(0, n_dp - 1)], m_recv.at[0])
    for t in range(1, 2 * n_z):
        remote(meta.at[me], meta.at[me], sent.at[5], m_recv.at[1], (dp, (me + t) % (2 * n_z))).start()
    wait_bytes(meta.at[pl.ds(0, 2 * n_z - 1)], m_recv.at[1])

    @pl.loop(0, 2 * n_z)
    def _(e):
        for d in range(n_dp):
            column = meta[e, d].T
            for j in range(n_j):
                at = pl.ds(pl.multiple_of((d * 2 + e % 2) * rows, rows), rows)
                facts_col[j * n_z + e // 2, at, :] = column[j * rows : (j + 1) * rows, :]

    def send_ahead(t):
        @pl.when(jnp.logical_and(t >= LEAD, t < chunks))
        def _():
            stage_a(t)

    def send_downs(t):
        ahead = t - DOWN_AT

        @pl.when(jnp.logical_and(ahead >= 0, jnp.logical_and(ahead < experts * DOWN_STEP, ahead % DOWN_STEP == 0)))
        def _():
            send_down(ahead // DOWN_STEP)

    steps = {
        "a": send_ahead,
        "b": lambda t: even(t, LAG_B, stage_b),
        "down": send_downs,
        "c": lambda t: even(t, LAG_C, stage_c),
        "g": lambda t: even(t, LAG_G, stage_g),
        "ra": lambda t: even(t, LAG_G + LAG_R[0], stage_ra),
        "rb": lambda t: even(t, LAG_G + LAG_R[1], stage_rb),
        "rc": lambda t: even(t, LAG_G + LAG_R[2], stage_rc),
        "rd": lambda t: even(t, LAG_G + LAG_R[3], stage_rd, TAIL),
        "re": lambda t: even(t, LAG_G + LAG_R[4], stage_re, TAIL),
        "m": lambda t: paced(t, 0, stage_m),
        "o1": lambda t: paced(t, LAG_O[0], stage_o1),
        "o2": lambda t: paced(t, LAG_O[1], stage_o2),
        "o3": lambda t: paced(t, LAG_O[2], stage_o3),
    }

    @pl.loop(min(LEAD, LAG_B), chunks + LAG_M + LAG_O[2])
    def _(t):
        for name in ORDER:
            steps[name](t)

    for j in range(n_j):
        for t in range(1, n_z):
            i = j * n_z + (z + t) % n_z
            wait_bytes(land.at[i], out_recv.at[i])
        for t in range(n_z):
            for d in range(n_dp):
                out_ref[j * rows : (j + 1) * rows, home(t, d) : home(t, d) + wide] = land[
                    j * n_z + t, :, d * wide : (d + 1) * wide
                ]

    for a in range(2):
        wait_bytes(weights.at[:, 0 : (n_spot - 1) * block, 0:unit], sent.at[a])
    wait_bytes(downs.at[0 : (n_spot - 1) * block, :], sent.at[2])
    wait_bytes(pieces.at[0 : n_z - 1], sent.at[3])
    wait_bytes(meta.at[0, 0 : n_dp - 1], sent.at[4])
    wait_bytes(meta.at[0 : 2 * n_z - 1], sent.at[5])
    wait_bytes(grid.at[:, 0:3], sent.at[6])
    wait_bytes(grid.at[0:LEAD, 0], sent.at[6])
    wait_bytes(grid.at[:, 0:2], sent.at[7])
    wait_bytes(grid.at[LEAD:chunks, 0], sent.at[7])
    wait_bytes(grid.at[:, 0], sent.at[8])

    @at_end
    def _():
        wait_bytes(part_out.at[:, 0], sent.at[9])
        wait_bytes(hidden.at[:, 0], sent.at[10])
        wait_bytes(hidden.at[TAIL:chunks], sent.at[10])

    @at_mid
    def _():
        wait_bytes(part_out, sent.at[9])
        wait_bytes(hidden.at[0:TAIL], sent.at[10])

    wait_bytes(from_core, sent.at[11])
    wait_bytes(from_first, sent.at[12])
    wait_bytes(from_second, sent.at[13])
    wait_bytes(final.at[0 : chunks - n_j], sent.at[14])


def shards(
    n_z, rows, tokens, routes, router_weight, shift, scale, gate_mod, gate_weight, up_weight, down_weight
):
    tok_dev, width = tokens.shape
    experts, depth, units = gate_weight.shape
    n_spot = width // (depth * n_z)
    n_dp = n_spot // 2
    dset = n_spot * depth
    unit = units // n_spot
    chunks = n_z * tok_dev // rows
    total = n_spot * rows
    vmem = pl.BlockSpec(memory_space=pltpu.VMEM)
    hbm = pl.BlockSpec(memory_space=pl.ANY)
    dma = pltpu.SemaphoreType.DMA
    return pl.pallas_call(
        kernel,
        out_shape=jax.ShapeDtypeStruct((tok_dev, width), BF16),
        in_specs=[vmem] * 6 + [hbm] * 3,
        out_specs=vmem,
        scratch_shapes=[
            pltpu.VMEM((n_z, tok_dev, dset), BF16),
            pltpu.VMEM((chunks, n_spot, rows, dset), BF16),
            pltpu.VMEM((experts, dset, 2 * unit), BF16),
            pltpu.VMEM((dset, experts * unit), BF16),
            pltpu.VMEM((2 * n_z, n_dp, 8, tok_dev), F32),
            pltpu.VMEM((chunks, total, 8), F32),
            pltpu.VMEM((HOLD, 2, total, 2 * unit), F32),
            pltpu.VMEM((chunks, 2, total, 2 * unit), BF16),
            pltpu.VMEM((chunks, 2, total, 2 * unit), BF16),
            pltpu.VMEM((chunks, 2, total, unit), BF16),
            pltpu.VMEM((total, experts * unit), BF16),
            pltpu.VMEM((RING, n_dp, rows, dset), F32),
            pltpu.VMEM((chunks, n_dp, rows, dset), BF16),
            pltpu.VMEM((chunks, n_dp, rows, dset), BF16),
            pltpu.VMEM((RING, 2, rows, dset), F32),
            pltpu.VMEM((chunks, 2, rows, dset), BF16),
            pltpu.VMEM((chunks, 2, rows, dset), BF16),
            pltpu.VMEM((RING, rows, dset), F32),
            pltpu.VMEM((chunks, rows, dset), BF16),
            pltpu.VMEM((chunks, rows, dset), BF16),
            pltpu.VMEM((chunks, rows, dset), BF16),
            pltpu.VMEM((chunks, rows, dset), BF16),
            pltpu.VMEM((1, dset), F32),
            dma((15,)),
            dma((3,)),
            dma((2,)),
            dma((chunks,)),
            dma((chunks,)),
            dma((chunks,)),
            dma((chunks,)),
            dma((chunks,)),
            dma((chunks, 2, 2)),
            dma((chunks, 2, 2)),
            dma((chunks,)),
            dma((chunks, 2)),
            dma((chunks,)),
            dma((chunks,)),
        ],
        compiler_params=pltpu.CompilerParams(
            collective_id=0, has_side_effects=True, vmem_limit_bytes=65000 * 1024
        ),
    )(tokens, router_weight.T, routes.T, shift, scale, gate_mod, gate_weight, up_weight, down_weight)


def choose(mesh):
    n_dp, n_owner = mesh.shape["dp"], mesh.shape["expert"]

    def body(*args):
        tokens, shift, weight = args[0], args[3], args[6]
        n_spot = 2 * n_dp
        fits = n_dp == 4 and n_owner == 8 and shift.shape[0] == 1
        fits = fits and tokens.shape[0] == 128 and tokens.shape[1] == n_dp * n_owner * weight.shape[1]
        fits = fits and weight.shape[1] % 128 == 0 and weight.shape[2] == 128 * n_spot and weight.shape[0] <= 8
        if fits:
            return shards(n_owner // 2, ROWS, *args)
        return shards_plain(*args)

    return body


def solution(mesh):
    in_specs = (
        P(("dp", "expert"), None),
        P(("dp", "expert"), None),
        P(),
        P(),
        P(),
        P(),
        P(None, ("dp", "expert"), None),
        P(None, ("dp", "expert"), None),
        P(None, ("dp", "expert"), None),
    )
    out_specs = P(("dp", "expert"), None)
    return jax.shard_map(
        choose(mesh), mesh=mesh, in_specs=in_specs, out_specs=out_specs, check_vma=False)
```
